32 devices in a mesh: dp: 8 (over y, z), tp: 4 (over x, core).
Axes of the slice: x: 2, y: 2, z: 4, core: 2. Of those that a mesh axis runs over, the one named last changes fastest.
Arguments:
- x: bfloat16 [8, 2048, 1536], P('dp', 'tp')
- dy: bfloat16 [8, 2048, 1536], P('dp', 'tp')
- wq: bfloat16 [1536, 1536], P('dp', 'tp')
- wk: bfloat16 [1536, 1536], P('dp', 'tp')
- wv: bfloat16 [1536, 1536], P('dp', 'tp')
- wo: bfloat16 [1536, 1536], P(('tp', 'dp'))
- w_gate: bfloat16 [1536, 6144], P('dp', 'tp')
- w_up: bfloat16 [1536, 6144], P('dp', 'tp')
- w_down: bfloat16 [6144, 1536], P(('tp', 'dp'))
Outputs:
- output 1: bfloat16 [8, 2048, 1536], P('dp', 'tp')
- output 2: bfloat16 [1536, 1536], P('dp', 'tp')
- output 3: bfloat16 [1536, 1536], P('dp', 'tp')
- output 4: bfloat16 [1536, 1536], P('dp', 'tp')
- output 5: bfloat16 [1536, 1536], P(('tp', 'dp'))
- output 6: bfloat16 [1536, 6144], P('dp', 'tp')
- output 7: bfloat16 [1536, 6144], P('dp', 'tp')
- output 8: bfloat16 [6144, 1536], P(('tp', 'dp'))
All inputs are finite; a program needn't handle non-finite values.
Results may differ from the reference program's by a relative error of at most 0.024.
Values are sent between devices in bfloat16 or wider.
A program may use at most 2 GiB of HBM per device.

```python
import jax
import jax.numpy as jnp
from jax import lax

SEQUENCES = 8
TOKENS = 2048
D = 1536
HEADS = 12
KV_HEADS = 12
HEAD = 128
FF = 6144
THETA = 10000
NAMES = ("wq", "wk", "wv", "wo", "w_gate", "w_up", "w_down")
SHAPES = {
    "wq": (D, HEADS * HEAD),
    "wk": (D, KV_HEADS * HEAD),
    "wv": (D, KV_HEADS * HEAD),
    "wo": (HEADS * HEAD, D),
    "w_gate": (D, FF),
    "w_up": (D, FF),
    "w_down": (FF, D),
}


def bump(key, n, height):
    away = (jnp.arange(n, dtype=jnp.int32) - jax.random.randint(key, (), 0, n, jnp.int32)) % n
    return jnp.where(away < n // 8, height, 1.0)


def together(key, own, strength):
    shared = jax.random.normal(key, own.shape[1:], jnp.float32)
    return (own + strength * shared) * lax.rsqrt(1 + strength * strength)


def setup_inputs(seed: int = 0, part: int = 0) -> dict:
    kx, kdy, ka, kb, kz, kf, kh, kl, *kw = jax.random.split(jax.random.key(seed), 8 + len(NAMES))
    shape = (SEQUENCES, TOKENS, D)
    much_x, much_dy = jax.random.uniform(kz, (2,), jnp.float32, 0.0, 1.0)
    loud = 2.0 ** jax.random.uniform(jax.random.fold_in(kz, 1), (), jnp.float32, -1.0, 2.0)
    halves = 2.0 ** jax.random.uniform(kl, (2,), jnp.float32, -1.0, 1.0)
    times = {"wq": 1.0, "wk": 1.0, "wv": 2.0, "wo": halves[0], "w_gate": 1.0, "w_up": bump(kh, FF, 4.0), "w_down": halves[1]}
    x = together(ka, jax.random.normal(kx, shape, jnp.float32), much_x) * bump(kf, D, 4.0)
    dy = together(kb, jax.random.normal(kdy, shape, jnp.float32), much_dy)
    drawn = {"x": x.astype(jnp.bfloat16), "dy": (loud * dy * (SEQUENCES * TOKENS) ** -0.5).astype(jnp.bfloat16)}
    for key, name in zip(kw, NAMES, strict=True):
        drawn[name] = (jax.random.normal(key, SHAPES[name], jnp.float32) * SHAPES[name][0] ** -0.5 * times[name]).astype(jnp.bfloat16)
    return drawn


def matmul(a, w):
    return jnp.dot(a, w, preferred_element_type=jnp.float32).astype(jnp.bfloat16)


def normed(h):
    wide = h.astype(jnp.float32)
    scale = lax.rsqrt(jnp.mean(wide**2, -1, keepdims=True) + 1e-6)
    return (wide * scale).astype(jnp.bfloat16)


def turned(t, theta):
    half = t.shape[-1] // 2
    angle = jnp.arange(t.shape[0], dtype=jnp.float32)[:, None] * theta ** (-jnp.arange(half, dtype=jnp.float32) / half)
    cos, sin = jnp.cos(angle)[:, None], jnp.sin(angle)[:, None]
    a, b = t[..., :half].astype(jnp.float32), t[..., half:].astype(jnp.float32)
    return jnp.concatenate([a * cos - b * sin, b * cos + a * sin], -1).astype(jnp.bfloat16)


def seen_by(q, k, v):
    tokens, kv = q.shape[0], k.shape[1]
    q = q.reshape(tokens, kv, -1, q.shape[-1])
    scores = jnp.einsum("tgsd,ugd->gstu", q.astype(jnp.float32), k.astype(jnp.float32)) * q.shape[-1] ** -0.5
    place = jnp.arange(tokens)
    weights = jax.nn.softmax(jnp.where(place[:, None] >= place, scores, -jnp.inf), -1).astype(jnp.bfloat16)
    return jnp.einsum("gstu,ugd->tgsd", weights.astype(jnp.float32), v.astype(jnp.float32)).astype(jnp.bfloat16).reshape(tokens, -1)


def layer(h, w):
    a = normed(h)
    q, k = (turned(matmul(a, w[name]).reshape(h.shape[0], -1, HEAD), THETA) for name in ("wq", "wk"))
    h = h + matmul(seen_by(q, k, matmul(a, w["wv"]).reshape(h.shape[0], -1, HEAD)), w["wo"])
    b = normed(h)
    gate = jnp.dot(b, w["w_gate"], preferred_element_type=jnp.float32)
    up = jnp.dot(b, w["w_up"], preferred_element_type=jnp.float32)
    return h + matmul((jax.nn.silu(gate) * up).astype(jnp.bfloat16), w["w_down"])


def reference(x, dy, wq, wk, wv, wo, w_gate, w_up, w_down):
    weights = dict(zip(NAMES, (wq, wk, wv, wo, w_gate, w_up, w_down), strict=True))

    def take(so_far, sequence):
        h, by_y = sequence
        _, back = jax.vjp(lambda w, h: layer(h, w), weights, h)
        by_weights, by_h = back(by_y)
        return jax.tree.map(lambda total, term: total + term.astype(jnp.float32), so_far, by_weights), by_h

    none_yet = {name: jnp.zeros(w.shape, jnp.float32) for name, w in weights.items()}
    by_weights, by_x = lax.scan(take, none_yet, (x, dy))
    return (by_x, *(by_weights[name].astype(jnp.bfloat16) for name in NAMES))
```

```python
import jax
import jax.numpy as jnp
from jax import lax
from jax.experimental import pallas as pl
from jax.experimental.pallas import tpu as pltpu
from jax.sharding import PartitionSpec as P


NEG = -1e30
HIDDEN = 2 * NEG
LOG2E = 1.4426950408889634
HEAD = 128
THETA = 10000
BLOCK = 512
VMEM = 56 * 2**20
F32, BF16 = jnp.float32, jnp.bfloat16


def dot(a, b, ca=1, cb=0):
    return lax.dot_general(a, b, (((ca,), (cb,)), ((), ())), preferred_element_type=F32)


def normed(h):
    wide = h.astype(F32)
    scale = lax.rsqrt(jnp.mean(wide**2, -1, keepdims=True) + 1e-6)
    return (wide * scale).astype(BF16)


def _mask():
    return lax.broadcasted_iota(jnp.int32, (BLOCK, BLOCK), 1) >= lax.broadcasted_iota(jnp.int32, (BLOCK, BLOCK), 0)


def _turn(t, cos, sin):
    return t * cos + pltpu.roll(t, HEAD // 2, 1) * sin


def _attend(me_ref, qkv_ref, cos_ref, sin_ref, o_ref, rot_ref, lse_ref, k_s, v_s, top_s, mix_s, *, heads):
    iq = pl.program_id(0)
    cos, sin = cos_ref[...], sin_ref[...]
    scale = HEAD**-0.5
    e = scale * LOG2E
    wide = heads * HEAD
    ones = jnp.ones((8, BLOCK), BF16)
    for i in range(heads):
        at = i * HEAD
        q = _turn(qkv_ref[:, at : at + HEAD].astype(F32), cos, sin).astype(BF16)
        k = _turn(qkv_ref[:, wide + at : wide + at + HEAD].astype(F32), cos, sin).astype(BF16)
        v = qkv_ref[:, 2 * wide + at : 2 * wide + at + HEAD]
        rot_ref[:, at : at + HEAD] = q
        rot_ref[:, wide + at : wide + at + HEAD] = k
        rot_ref[:, 2 * wide + at : 2 * wide + at + HEAD] = v
        k_s[iq, :, at : at + HEAD] = k
        v_s[iq, i] = jnp.concatenate([v.T, ones], axis=0)
        top_s[i : i + 1, :] = jnp.full((1, BLOCK), NEG, F32)
        mix_s[i] = jnp.zeros((HEAD + 8, BLOCK), F32)

    def block(j, masked):
        scores = [dot(k_s[j, :, i * HEAD : (i + 1) * HEAD], rot_ref[:, i * HEAD : (i + 1) * HEAD], 1, 1) for i in range(heads)]
        ok = _mask() if masked else None
        weights, keeps = [], []
        for i, s in enumerate(scores):
            if masked:
                s = jnp.where(ok, s, HIDDEN)
            old = top_s[i : i + 1, :]
            top = jnp.maximum(old, s.max(axis=0, keepdims=True))
            top_s[i : i + 1, :] = top
            weights.append(jnp.exp2((s - top) * e).astype(BF16))
            keeps.append(jnp.exp2((old - top) * e))
        for i in range(heads):
            mix_s[i] = mix_s[i] * keeps[i] + dot(v_s[j, i], weights[i], 1, 0)

    lax.fori_loop(0, iq, lambda j, _: block(j, False), None)
    block(iq, True)
    for i in range(heads):
        total = mix_s[i, HEAD : HEAD + 1, :]
        o_ref[:, i * HEAD : (i + 1) * HEAD] = (mix_s[i, :HEAD, :] * (1 / total)).T.astype(BF16)
        lse_ref[i : i + 1, :] = top_s[i : i + 1, :] * scale + jnp.log(total)


def attend(me, qkv, cos, sin):
    tokens, width = qkv.shape
    heads = width // (3 * HEAD)
    n = tokens // BLOCK
    here = lambda t, me: (t ^ me[0], 0)
    return pl.pallas_call(
        lambda *refs: _attend(*refs, heads=heads),
        grid_spec=pltpu.PrefetchScalarGridSpec(
            num_scalar_prefetch=1,
            grid=(n,),
            in_specs=[pl.BlockSpec((BLOCK, width), here), pl.BlockSpec((BLOCK, HEAD), lambda t, me: (t, 0)),
                      pl.BlockSpec((BLOCK, HEAD), lambda t, me: (t, 0))],
            out_specs=[pl.BlockSpec((BLOCK, heads * HEAD), here), pl.BlockSpec((BLOCK, width), here),
                       pl.BlockSpec((heads, BLOCK), lambda t, me: (0, t ^ me[0]))],
            scratch_shapes=[pltpu.VMEM((n, BLOCK, heads * HEAD), BF16), pltpu.VMEM((n, heads, HEAD + 8, BLOCK), BF16),
                            pltpu.VMEM((heads, BLOCK), F32), pltpu.VMEM((heads, HEAD + 8, BLOCK), F32)],
        ),
        out_shape=[jax.ShapeDtypeStruct((tokens, heads * HEAD), BF16), jax.ShapeDtypeStruct(qkv.shape, BF16),
                   jax.ShapeDtypeStruct((heads, tokens), F32)],
        compiler_params=pltpu.CompilerParams(dimension_semantics=("arbitrary",), vmem_limit_bytes=VMEM),
        cost_estimate=pl.CostEstimate(flops=2 * heads * tokens * tokens * HEAD * 3, transcendentals=heads * tokens * tokens // 2,
                                      bytes_accessed=tokens * width * 5),
    )(me, qkv, cos, sin)


def _attend_bwd(me_ref, rot_ref, o_ref, do_ref, lse_ref, cos_ref, sin_ref, out_ref, dq_s, dk_s, dv_s, *, heads, n):
    t = pl.program_id(0)
    iq = n - 1 - t
    me = me_ref[0]
    cos, sin = cos_ref[...], sin_ref[...]
    scale = HEAD**-0.5
    e = scale * LOG2E
    wide = heads * HEAD

    @pl.when(t == 0)
    def _():
        dk_s[...] = jnp.zeros_like(dk_s)
        dv_s[...] = jnp.zeros_like(dv_s)

    dq_s[...] = jnp.zeros_like(dq_s)
    mine = pl.ds((iq ^ me) * BLOCK, BLOCK)
    lses, deltas = [], []
    for i in range(heads):
        cut = slice(i * HEAD, (i + 1) * HEAD)
        lses.append(lse_ref[i : i + 1, :] * LOG2E)
        deltas.append((do_ref[:, cut].astype(F32) * o_ref[:, cut].astype(F32)).T.sum(axis=0, keepdims=True))

    def block(j, masked):
        keys = pl.ds((j ^ me) * BLOCK, BLOCK)
        cuts = [slice(i * HEAD, (i + 1) * HEAD) for i in range(heads)]
        qs = [rot_ref[mine, c] for c in cuts]
        ks = [rot_ref[keys, wide + i * HEAD : wide + (i + 1) * HEAD] for i in range(heads)]
        vs = [rot_ref[keys, 2 * wide + i * HEAD : 2 * wide + (i + 1) * HEAD] for i in range(heads)]
        scores = [dot(k, q, 1, 1) for k, q in zip(ks, qs)]
        dps = [dot(v, do_ref[:, c], 1, 1) for v, c in zip(vs, cuts)]
        ok = _mask() if masked else None
        for i in range(heads):
            p = jnp.exp2(scores[i] * e - lses[i])
            if masked:
                p = jnp.where(ok, p, 0.0)
            ds = (p * (dps[i] - deltas[i])).astype(BF16)
            dv_s[j, :, cuts[i]] += dot(p.astype(BF16), do_ref[:, cuts[i]], 1, 0)
            dk_s[j, :, cuts[i]] += dot(ds, qs[i], 1, 0)
            dq_s[i] += dot(ks[i].T, ds, 1, 0)

    lax.fori_loop(0, iq, lambda j, _: block(j, False), None)
    block(iq, True)
    for i in range(heads):
        cut = slice(i * HEAD, (i + 1) * HEAD)
        dq = (dq_s[i] * scale).T
        dk = dk_s[iq, :, cut] * scale
        out_ref[:, cut] = _turn(dq, cos, -sin).astype(BF16)
        out_ref[:, wide + i * HEAD : wide + (i + 1) * HEAD] = _turn(dk, cos, -sin).astype(BF16)
        out_ref[:, 2 * wide + i * HEAD : 2 * wide + (i + 1) * HEAD] = dv_s[iq, :, cut].astype(BF16)


def attend_bwd(me, rot, o, do, lse, cos, sin):
    tokens, width = rot.shape
    heads = width // (3 * HEAD)
    n = tokens // BLOCK
    here = lambda t, me: ((n - 1 - t) ^ me[0], 0)
    table = pl.BlockSpec((BLOCK, HEAD), lambda t, me: (n - 1 - t, 0))
    return pl.pallas_call(
        lambda *refs: _attend_bwd(*refs, heads=heads, n=n),
        grid_spec=pltpu.PrefetchScalarGridSpec(
            num_scalar_prefetch=1,
            grid=(n,),
            in_specs=[pl.BlockSpec((tokens, width), lambda t, me: (0, 0)), pl.BlockSpec((BLOCK, heads * HEAD), here),
                      pl.BlockSpec((BLOCK, heads * HEAD), here), pl.BlockSpec((heads, BLOCK), lambda t, me: (0, (n - 1 - t) ^ me[0])),
                      table, table],
            out_specs=pl.BlockSpec((BLOCK, width), here),
            scratch_shapes=[pltpu.VMEM((heads, HEAD, BLOCK), F32), pltpu.VMEM((n, BLOCK, heads * HEAD), F32),
                            pltpu.VMEM((n, BLOCK, heads * HEAD), F32)],
        ),
        out_shape=jax.ShapeDtypeStruct((tokens, width), BF16),
        compiler_params=pltpu.CompilerParams(dimension_semantics=("arbitrary",), vmem_limit_bytes=VMEM),
        cost_estimate=pl.CostEstimate(flops=2 * heads * tokens * tokens * HEAD * 4, transcendentals=heads * tokens * tokens // 2,
                                      bytes_accessed=tokens * width * 5),
    )(me, rot, o, do, lse, cos, sin)


def _gated(b_ref, wg_ref, wu_ref, dh_ref, hid_ref, dg_ref, du_ref):
    rows = pl.ds(pl.multiple_of(pl.program_id(1) * BLOCK, BLOCK), BLOCK)
    b = b_ref[rows, :]
    gate, up = dot(b, wg_ref[...]), dot(b, wu_ref[...])
    dh = dh_ref[...].astype(F32)
    sig = 1 / (1 + jnp.exp(-gate))
    silu = gate * sig
    hid_ref[...] = (silu * up).astype(BF16)
    du_ref[...] = (dh * silu).astype(BF16)
    dg_ref[...] = (dh * up * (sig * (1 + gate * (1 - sig)))).astype(BF16)


def gated(b, wgu, dhid):
    tokens, d = b.shape
    ff = dhid.shape[1]
    tile = 512
    nt = ff // tile
    out = pl.BlockSpec((BLOCK, tile), lambda n, m: (m, n))
    return pl.pallas_call(
        _gated,
        grid=(nt, tokens // BLOCK),
        in_specs=[pl.BlockSpec((tokens, d), lambda n, m: (0, 0)), pl.BlockSpec((d, tile), lambda n, m: (0, n)),
                  pl.BlockSpec((d, tile), lambda n, m: (0, n + nt)), out],
        out_specs=[out, out, out],
        out_shape=[jax.ShapeDtypeStruct((tokens, ff), BF16)] * 3,
        compiler_params=pltpu.CompilerParams(dimension_semantics=("arbitrary", "arbitrary"), vmem_limit_bytes=VMEM),
        cost_estimate=pl.CostEstimate(flops=4 * tokens * d * ff, transcendentals=tokens * ff, bytes_accessed=2 * (tokens * d + 2 * d * ff + 4 * tokens * ff)),
    )(b, wgu, wgu, dhid)


RING = [0, 1, 2, 3, 7, 6, 5, 4]
RIGHT = [(RING[i], RING[(i + 1) % 8]) for i in range(8)]
LEFT = [(b, a) for a, b in RIGHT]
ACROSS = [(i, i ^ 2) for i in range(4)]
BESIDE = [(i, i ^ 1) for i in range(4)]


def ring(q):
    q = lax.rem(q + 16, 8)
    return jnp.where(q < 4, q, 11 - q)


def right(v):
    return lax.ppermute(v, "dp", RIGHT)


def left(v):
    return lax.ppermute(v, "dp", LEFT)


def collect(block):
    half = block.shape[0] // 2 // 16 * 16
    r = l = block
    got = [(0, 0, block)]
    for s in (1, 2, 3):
        r, l = right(r), left(l)
        got += [(-s, 0, r), (s, 0, l)]
    got += [(4, 0, right(r[:half])), (4, half, left(l[half:]))]
    return got


def laid(pos, got, rows):
    out = jnp.zeros((8 * rows, got[0][2].shape[1]), BF16)
    for far, first, part in got:
        out = lax.dynamic_update_slice(out, part, (ring(pos + far) * rows + first, jnp.int32(0)))
    return out


def scatter(pos, total):
    rows = total.shape[0] // 8
    half = rows // 2 // 16 * 16
    term = lambda far: lax.dynamic_slice(total, (ring(pos + far) * rows, jnp.int32(0)), (rows, total.shape[1]))
    add = lambda a, b: (a.astype(F32) + b.astype(F32)).astype(BF16)
    t = term(4)
    r, l = right(t[:half]), left(t[half:])
    a, b = term(3), term(-3)
    r = right(jnp.concatenate([add(r, a[:half]), a[half:]]))
    l = left(jnp.concatenate([b[:half], add(l, b[half:])]))
    for s in (2, 1):
        r, l = right(add(r, term(s))), left(add(l, term(-s)))
    return (term(0).astype(F32) + r.astype(F32) + l.astype(F32)).astype(BF16)


def across(v):
    return lax.ppermute(v, "tp", ACROSS)


def beside(v):
    return lax.ppermute(v, "tp", BESIDE)


def gathered(v):
    far = across(v)
    return jnp.concatenate([v, beside(v), far, beside(far)])


def summed(near, far):
    pair = beside(far[BLOCK:]).astype(F32) + far[:BLOCK].astype(F32)
    pair = across(pair.astype(BF16))
    return near[:BLOCK].astype(F32) + beside(near[BLOCK:]).astype(F32) + pair.astype(F32)


def step(x, dy, wq, wk, wv, wo, w_gate, w_up, w_down):
    x, dy = x[0], dy[0]
    me = lax.axis_index("tp").astype(jnp.int32)
    pos = ring(lax.axis_index("dp").astype(jnp.int32))
    who = me[None]
    n_qkv, n_wo = wq.shape[0], wo.shape[0]

    wqkv = laid(pos, collect(jnp.concatenate([wq, wk, wv], 1)), n_qkv)
    a, norm_a = jax.vjp(normed, x)
    a = gathered(a)
    place = jnp.arange(4 * BLOCK, dtype=F32)[:, None] * THETA ** (-jnp.arange(HEAD // 2, dtype=F32) / (HEAD // 2))
    cos, sin = jnp.cos(place), jnp.sin(place)
    cos, sin = jnp.concatenate([cos, cos], 1), jnp.concatenate([-sin, sin], 1)

    rows = collect(jnp.concatenate([wo, w_down]))
    gu = collect(jnp.concatenate([w_gate, w_up], 1))
    half = rows[-2][2].shape[0]
    wo_parts = [(f, 0, v[:n_wo]) for f, first, v in rows if first == 0]
    wd_parts = [(f, 0, v[n_wo:]) for f, first, v in rows[:-1]] + [(rows[-1][0], half - n_wo, rows[-1][2])]
    wo_full = laid(pos, wo_parts, n_wo)
    wd_full = laid(pos, wd_parts, w_down.shape[0])
    wgu = laid(pos, gu, w_gate.shape[0])

    qkv = dot(a, wqkv).astype(BF16)
    heads, rot, lse = attend(who, qkv, cos, sin)
    far = dot(heads[2 * BLOCK :], wo_full).astype(BF16)
    near = dot(heads[: 2 * BLOCK], wo_full).astype(BF16)
    h = x + summed(near, far).astype(BF16)
    b, norm_b = jax.vjp(normed, h)
    b = gathered(b)
    dyf = gathered(dy)
    dhid = dot(dyf, wd_full, 1, 1).astype(BF16)
    hid, dgate, dup = gated(b, wgu, dhid)
    dgu = jnp.concatenate([dgate, dup], 1)
    far = dot(dgu[2 * BLOCK :], wgu, 1, 1).astype(BF16)
    near = dot(dgu[: 2 * BLOCK], wgu, 1, 1).astype(BF16)
    by_down = scatter(pos, dot(hid, dyf, 0, 0).astype(BF16))
    by_gu = scatter(pos, dot(b, dgu, 0, 0).astype(BF16))
    dh = dy + norm_b(summed(near, far).astype(BF16))[0]
    dhf = gathered(dh)
    dheads = dot(dhf, wo_full, 1, 1).astype(BF16)
    by_wo = scatter(pos, dot(heads, dhf, 0, 0).astype(BF16))
    dqkv = attend_bwd(who, rot, heads, dheads, lse, cos, sin)
    far = dot(dqkv[2 * BLOCK :], wqkv, 1, 1).astype(BF16)
    near = dot(dqkv[: 2 * BLOCK], wqkv, 1, 1).astype(BF16)
    by_qkv = scatter(pos, dot(a, dqkv, 0, 0).astype(BF16))
    dx = dh + norm_a(summed(near, far).astype(BF16))[0]
    c, f = wq.shape[1], w_gate.shape[1]
    return (dx[None], by_qkv[:, :c], by_qkv[:, c : 2 * c], by_qkv[:, 2 * c :], by_wo, by_gu[:, :f], by_gu[:, f:], by_down)


def solution(mesh):
    states, by_columns, by_rows = P("dp", "tp", None), P("dp", "tp"), P(("tp", "dp"), None)
    weights = (by_columns, by_columns, by_columns, by_rows, by_columns, by_columns, by_rows)
    return jax.shard_map(step, mesh=mesh, in_specs=(states, states, *weights), out_specs=(states, *weights), check_vma=False)
```

```python
import functools

import jax
import jax.numpy as jnp
from jax import lax
from jax.experimental import pallas as pl
from jax.experimental.pallas import tpu as pltpu
from jax.sharding import PartitionSpec as P


NEG = -1e30
HIDDEN = 2 * NEG
LOG2E = 1.4426950408889634
HEAD = 128
THETA = 10000
BLOCK = 512
VMEM = 56 * 2**20
F32, BF16 = jnp.float32, jnp.bfloat16


def dot(a, b, ca=1, cb=0):
    return lax.dot_general(a, b, (((ca,), (cb,)), ((), ())), preferred_element_type=F32)


def normed(h):
    wide = h.astype(F32)
    scale = lax.rsqrt(jnp.mean(wide**2, -1, keepdims=True) + 1e-6)
    return (wide * scale).astype(BF16)


def _mask():
    return lax.broadcasted_iota(jnp.int32, (BLOCK, BLOCK), 1) >= lax.broadcasted_iota(jnp.int32, (BLOCK, BLOCK), 0)


def _turn(t, cos, sin):
    return t * cos + pltpu.roll(t, HEAD // 2, 1) * sin


RING = [0, 1, 2, 3, 7, 6, 5, 4]
PIECES = [(0, 0), (-1, 0), (1, 0), (-2, 0), (2, 0), (-3, 0), (3, 0), (4, 0), (4, 1)]


def ring(q):
    q = lax.rem(q + 16, 8)
    return jnp.where(q < 4, q, 11 - q)


def _half(rows):
    return rows // 2 // 16 * 16


def _place(refs, to, sems, pos, columns=None):
    rows = refs[0].shape[0]
    copies = []
    for n, (ref, (far, second)) in enumerate(zip(refs, PIECES)):
        at = pl.multiple_of(ring(pos + far) * rows + second * _half(rows), 16)
        source, target = (ref, to.at[pl.ds(at, ref.shape[0]), :])
        if columns is not None:
            source, target = ref.at[:, columns], to.at[pl.ds(at, ref.shape[0]), columns]
        copies.append(pltpu.make_async_copy(source, target, sems.at[n]))
    return copies


def _stack(refs, to, sems):
    return [pltpu.make_async_copy(ref, to.at[pl.ds(n * BLOCK, BLOCK), :], sems.at[n]) for n, ref in enumerate(refs)]


def _attend(at_ref, *refs, heads):
    a_refs, w_refs, p_refs = refs[:4], refs[4:13], refs[13:22]
    cos_ref, sin_ref, o_ref, rot_ref, lse_ref, a_out, w_out, p_out, a_s, w_s, p_s, k_s, v_s, top_s, mix_s, a_sem, w_sem, p_sem, out_sem = refs[22:]
    iq = pl.program_id(0)
    me, pos = at_ref[0], at_ref[1]
    scale = HEAD**-0.5
    e = scale * LOG2E
    wide = heads * HEAD
    keep = [pltpu.make_async_copy(a, b, out_sem.at[n]) for n, (a, b) in enumerate(((a_s, a_out), (w_s, w_out), (p_s, p_out)))]

    @pl.when(iq == 0)
    def _():
        copies = _stack(a_refs, a_s, a_sem) + _place(w_refs, w_s, w_sem, pos) + _place(p_refs, p_s, p_sem, pos)
        for c in copies:
            c.start()
        for c in copies:
            c.wait()
        for c in keep:
            c.start()

    rows = pl.ds(pl.multiple_of((iq ^ me) * BLOCK, BLOCK), BLOCK)
    qkv = dot(a_s[rows, :], w_s[...]).astype(BF16)
    cos, sin = cos_ref[...], sin_ref[...]
    ones = jnp.ones((8, BLOCK), BF16)
    for i in range(heads):
        at = i * HEAD
        q = _turn(qkv[:, at : at + HEAD].astype(F32), cos, sin).astype(BF16)
        k = _turn(qkv[:, wide + at : wide + at + HEAD].astype(F32), cos, sin).astype(BF16)
        v = qkv[:, 2 * wide + at : 2 * wide + at + HEAD]
        rot_ref[:, at : at + HEAD] = q
        rot_ref[:, wide + at : wide + at + HEAD] = k
        rot_ref[:, 2 * wide + at : 2 * wide + at + HEAD] = v
        k_s[iq, :, at : at + HEAD] = k
        v_s[iq, i] = jnp.concatenate([v.T, ones], axis=0)
        top_s[i : i + 1, :] = jnp.full((1, BLOCK), NEG, F32)
        mix_s[i] = jnp.zeros((HEAD + 8, BLOCK), F32)

    def block(j, masked):
        scores = [dot(k_s[j, :, i * HEAD : (i + 1) * HEAD], rot_ref[:, i * HEAD : (i + 1) * HEAD], 1, 1) for i in range(heads)]
        ok = _mask() if masked else None
        weights, keeps = [], []
        for i, s in enumerate(scores):
            if masked:
                s = jnp.where(ok, s, HIDDEN)
            old = top_s[i : i + 1, :]
            top = jnp.maximum(old, s.max(axis=0, keepdims=True))
            top_s[i : i + 1, :] = top
            weights.append(jnp.exp2((s - top) * e).astype(BF16))
            keeps.append(jnp.exp2((old - top) * e))
        for i in range(heads):
            mix_s[i] = mix_s[i] * keeps[i] + dot(v_s[j, i], weights[i], 1, 0)

    lax.fori_loop(0, iq, lambda j, _: block(j, False), None)
    block(iq, True)
    for i in range(heads):
        total = mix_s[i, HEAD : HEAD + 1, :]
        o_ref[:, i * HEAD : (i + 1) * HEAD] = (mix_s[i, :HEAD, :] * (1 / total)).T.astype(BF16)
        lse_ref[i : i + 1, :] = top_s[i : i + 1, :] * scale + jnp.log(total)

    @pl.when(iq == pl.num_programs(0) - 1)
    def _():
        for c in keep:
            c.wait()


ANY = pl.BlockSpec(memory_space=pl.ANY)


def attend(at, blocks, pieces, o_pieces, cos, sin):
    n, d = len(blocks), blocks[0].shape[1]
    deep = 8 * o_pieces[0].shape[0]
    tokens, width = n * BLOCK, pieces[0].shape[1]
    heads = width // (3 * HEAD)
    here = lambda t, at: (t ^ at[0], 0)
    table = pl.BlockSpec((BLOCK, HEAD), lambda t, at: (t, 0))
    return pl.pallas_call(
        lambda *refs: _attend(*refs, heads=heads),
        grid_spec=pltpu.PrefetchScalarGridSpec(
            num_scalar_prefetch=1,
            grid=(n,),
            in_specs=[ANY] * 22 + [table, table],
            out_specs=[pl.BlockSpec((BLOCK, heads * HEAD), here), pl.BlockSpec((BLOCK, width), here),
                       pl.BlockSpec((heads, BLOCK), lambda t, at: (0, t ^ at[0])), ANY, ANY, ANY],
            scratch_shapes=[pltpu.VMEM((tokens, d), BF16), pltpu.VMEM((d, width), BF16), pltpu.VMEM((deep, d), BF16),
                            pltpu.VMEM((n, BLOCK, heads * HEAD), BF16), pltpu.VMEM((n, heads, HEAD + 8, BLOCK), BF16),
                            pltpu.VMEM((heads, BLOCK), F32), pltpu.VMEM((heads, HEAD + 8, BLOCK), F32),
                            pltpu.SemaphoreType.DMA((4,)), pltpu.SemaphoreType.DMA((9,)), pltpu.SemaphoreType.DMA((9,)), pltpu.SemaphoreType.DMA((3,))],
        ),
        out_shape=[jax.ShapeDtypeStruct((tokens, heads * HEAD), BF16), jax.ShapeDtypeStruct((tokens, width), BF16),
                   jax.ShapeDtypeStruct((heads, tokens), F32), jax.ShapeDtypeStruct((tokens, d), BF16), jax.ShapeDtypeStruct((d, width), BF16),
                   jax.ShapeDtypeStruct((deep, d), BF16)],
        compiler_params=pltpu.CompilerParams(dimension_semantics=("arbitrary",), vmem_limit_bytes=VMEM),
        cost_estimate=pl.CostEstimate(flops=2 * heads * tokens * tokens * HEAD * 3 + 2 * tokens * d * width, transcendentals=heads * tokens * tokens // 2,
                                      bytes_accessed=tokens * width * 5),
    )(at, *blocks, *pieces, *o_pieces, cos, sin)


def _hidden_grad(at_ref, *refs):
    y_refs, w_refs, out_ref, y_out, y_s, w_s, y_sem, w_sem, out_sem = refs[:4], refs[4:13], *refs[13:]
    m = pl.program_id(0)
    keep = pltpu.make_async_copy(y_s, y_out, out_sem)

    @pl.when(m == 0)
    def _():
        copies = _stack(y_refs, y_s, y_sem) + _place(w_refs, w_s, w_sem, at_ref[1])
        for c in copies:
            c.start()
        for c in copies:
            c.wait()
        keep.start()

    rows = pl.ds(pl.multiple_of(m * BLOCK, BLOCK), BLOCK)
    y = y_s[rows, :]
    tile = 512
    for n in range(0, out_ref.shape[1], tile):
        out_ref[:, n : n + tile] = dot(y, w_s[n : n + tile, :], 1, 1).astype(BF16)

    @pl.when(m == pl.num_programs(0) - 1)
    def _():
        keep.wait()


def hidden_grad(at, blocks, pieces):
    d = blocks[0].shape[1]
    tokens, ff = 4 * BLOCK, 8 * pieces[0].shape[0]
    return pl.pallas_call(
        _hidden_grad,
        grid_spec=pltpu.PrefetchScalarGridSpec(
            num_scalar_prefetch=1, grid=(4,), in_specs=[ANY] * 13, out_specs=[pl.BlockSpec((BLOCK, ff), lambda m, at: (m, 0)), ANY],
            scratch_shapes=[pltpu.VMEM((tokens, d), BF16), pltpu.VMEM((ff, d), BF16),
                            pltpu.SemaphoreType.DMA((4,)), pltpu.SemaphoreType.DMA((9,)), pltpu.SemaphoreType.DMA(())]),
        out_shape=[jax.ShapeDtypeStruct((tokens, ff), BF16), jax.ShapeDtypeStruct((tokens, d), BF16)],
        compiler_params=pltpu.CompilerParams(dimension_semantics=("arbitrary",), vmem_limit_bytes=VMEM),
        cost_estimate=pl.CostEstimate(flops=2 * tokens * ff * d, transcendentals=0, bytes_accessed=2 * tokens * (ff + 2 * d)),
    )(at, *blocks, *pieces)


def _attend_bwd(me_ref, rot_ref, o_ref, do_ref, lse_ref, cos_ref, sin_ref, out_ref, dq_s, dk_s, dv_s, *, heads, n):
    t = pl.program_id(0)
    iq = n - 1 - t
    me = me_ref[0]
    cos, sin = cos_ref[...], sin_ref[...]
    scale = HEAD**-0.5
    e = scale * LOG2E
    wide = heads * HEAD

    @pl.when(t == 0)
    def _():
        dk_s[...] = jnp.zeros_like(dk_s)
        dv_s[...] = jnp.zeros_like(dv_s)

    dq_s[...] = jnp.zeros_like(dq_s)
    mine = pl.ds((iq ^ me) * BLOCK, BLOCK)
    lses, deltas = [], []
    for i in range(heads):
        cut = slice(i * HEAD, (i + 1) * HEAD)
        lses.append(lse_ref[i : i + 1, :] * LOG2E)
        deltas.append((do_ref[:, cut].astype(F32) * o_ref[:, cut].astype(F32)).T.sum(axis=0, keepdims=True))

    def block(j, masked):
        keys = pl.ds((j ^ me) * BLOCK, BLOCK)
        cuts = [slice(i * HEAD, (i + 1) * HEAD) for i in range(heads)]
        qs = [rot_ref[mine, c] for c in cuts]
        ks = [rot_ref[keys, wide + i * HEAD : wide + (i + 1) * HEAD] for i in range(heads)]
        vs = [rot_ref[keys, 2 * wide + i * HEAD : 2 * wide + (i + 1) * HEAD] for i in range(heads)]
        scores = [dot(k, q, 1, 1) for k, q in zip(ks, qs)]
        dps = [dot(v, do_ref[:, c], 1, 1) for v, c in zip(vs, cuts)]
        ok = _mask() if masked else None
        for i in range(heads):
            p = jnp.exp2(scores[i] * e - lses[i])
            if masked:
                p = jnp.where(ok, p, 0.0)
            ds = (p * (dps[i] - deltas[i])).astype(BF16)
            dv_s[j, :, cuts[i]] += dot(p.astype(BF16), do_ref[:, cuts[i]], 1, 0)
            dk_s[j, :, cuts[i]] += dot(ds, qs[i], 1, 0)
            dq_s[i] += dot(ks[i].T, ds, 1, 0)

    lax.fori_loop(0, iq, lambda j, _: block(j, False), None)
    block(iq, True)
    for i in range(heads):
        cut = slice(i * HEAD, (i + 1) * HEAD)
        dq = (dq_s[i] * scale).T
        dk = dk_s[iq, :, cut] * scale
        out_ref[:, cut] = _turn(dq, cos, -sin).astype(BF16)
        out_ref[:, wide + i * HEAD : wide + (i + 1) * HEAD] = _turn(dk, cos, -sin).astype(BF16)
        out_ref[:, 2 * wide + i * HEAD : 2 * wide + (i + 1) * HEAD] = dv_s[iq, :, cut].astype(BF16)


def attend_bwd(me, rot, o, do, lse, cos, sin):
    tokens, width = rot.shape
    heads = width // (3 * HEAD)
    n = tokens // BLOCK
    here = lambda t, me: ((n - 1 - t) ^ me[0], 0)
    table = pl.BlockSpec((BLOCK, HEAD), lambda t, me: (n - 1 - t, 0))
    return pl.pallas_call(
        lambda *refs: _attend_bwd(*refs, heads=heads, n=n),
        grid_spec=pltpu.PrefetchScalarGridSpec(
            num_scalar_prefetch=1,
            grid=(n,),
            in_specs=[pl.BlockSpec((tokens, width), lambda t, me: (0, 0)), pl.BlockSpec((BLOCK, heads * HEAD), here),
                      pl.BlockSpec((BLOCK, heads * HEAD), here), pl.BlockSpec((heads, BLOCK), lambda t, me: (0, (n - 1 - t) ^ me[0])),
                      table, table],
            out_specs=pl.BlockSpec((BLOCK, width), here),
            scratch_shapes=[pltpu.VMEM((heads, HEAD, BLOCK), F32), pltpu.VMEM((n, BLOCK, heads * HEAD), F32),
                            pltpu.VMEM((n, BLOCK, heads * HEAD), F32)],
        ),
        out_shape=jax.ShapeDtypeStruct((tokens, width), BF16),
        compiler_params=pltpu.CompilerParams(dimension_semantics=("arbitrary",), vmem_limit_bytes=VMEM),
        cost_estimate=pl.CostEstimate(flops=2 * heads * tokens * tokens * HEAD * 4, transcendentals=heads * tokens * tokens // 2,
                                      bytes_accessed=tokens * width * 5),
    )(me, rot, o, do, lse, cos, sin)


def _gated(at_ref, *refs, second):
    b_refs, w_refs, dh_ref, rest = refs[:4], refs[4:13], refs[13], refs[14 + 2 * second :]
    hid_ref, dgu_ref, w_out, *b_out, b_s, w_s, b_sem, w_sem, out_sem = rest
    m = pl.program_id(0)
    half, wide = dh_ref.shape[1], w_s.shape[1]
    blocks = _stack(b_refs, b_s, b_sem)
    weights = _place(w_refs, w_s, w_sem, at_ref[1])
    keep = [pltpu.make_async_copy(w_s, w_out.at[:, second * wide : (second + 1) * wide], out_sem.at[0])]
    late = [pltpu.make_async_copy(b_s, out, out_sem.at[1]) for out in b_out]

    @pl.when(m == 0)
    def _():
        for c in [blocks[0]] + weights + blocks[1:]:
            c.start()
        for c in weights:
            c.wait()
        for c in keep:
            c.start()

    for k, c in enumerate(blocks):

        @pl.when(m == k)
        def _():
            c.wait()
            if k == len(blocks) - 1:
                for o in late:
                    o.start()

    part = BLOCK // 2
    for i in range(2):
        here = slice(i * part, (i + 1) * part)
        both = dot(b_s[pl.ds(pl.multiple_of(m * BLOCK + i * part, part), part), :], w_s[...])
        gate, up = both[:, :half], both[:, half:]
        dh = dh_ref[here, :].astype(F32)
        sig = 1 / (1 + jnp.exp(-gate))
        silu = gate * sig
        hid_ref[here, :] = (silu * up).astype(BF16)
        dgu_ref[here, :half] = (dh * up * (sig * (1 + gate * (1 - sig)))).astype(BF16)
        dgu_ref[here, half:] = (dh * silu).astype(BF16)

    @pl.when(m == pl.num_programs(0) - 1)
    def _():
        for c in keep + late:
            c.wait()


def gated(at, blocks, pieces, dhid, earlier=()):
    d, (tokens, ff) = blocks[0].shape[1], dhid.shape
    second, half = len(earlier) // 2, ff // 2
    outs = [jax.ShapeDtypeStruct((tokens, half), BF16), jax.ShapeDtypeStruct((tokens, 2 * ff), BF16), jax.ShapeDtypeStruct((d, 2 * ff), BF16)]
    outs += [] if second else [jax.ShapeDtypeStruct((tokens, d), BF16)]
    return pl.pallas_call(
        functools.partial(_gated, second=second),
        grid_spec=pltpu.PrefetchScalarGridSpec(
            num_scalar_prefetch=1,
            grid=(tokens // BLOCK,),
            in_specs=[ANY] * 13 + [pl.BlockSpec((BLOCK, half), lambda m, at: (m, second))] + [ANY] * len(earlier),
            out_specs=[pl.BlockSpec((BLOCK, half), lambda m, at: (m, 0)), pl.BlockSpec((BLOCK, ff), lambda m, at: (m, second))] + [ANY] * (len(outs) - 2),
            scratch_shapes=[pltpu.VMEM((tokens, d), BF16), pltpu.VMEM((d, ff), BF16),
                            pltpu.SemaphoreType.DMA((4,)), pltpu.SemaphoreType.DMA((9,)), pltpu.SemaphoreType.DMA((2,))],
        ),
        out_shape=outs,
        input_output_aliases={15 + n: 1 + n for n in range(len(earlier))},
        compiler_params=pltpu.CompilerParams(dimension_semantics=("arbitrary",), vmem_limit_bytes=VMEM),
        cost_estimate=pl.CostEstimate(flops=2 * tokens * d * ff, transcendentals=tokens * half, bytes_accessed=2 * (tokens * d + d * ff + 2 * tokens * ff)),
    )(at, *blocks, *pieces, dhid, *earlier)


RIGHT = [(RING[i], RING[(i + 1) % 8]) for i in range(8)]
LEFT = [(b, a) for a, b in RIGHT]
ACROSS = [(i, i ^ 2) for i in range(4)]
BESIDE = [(i, i ^ 1) for i in range(4)]


def right(v):
    return lax.ppermute(v, "dp", RIGHT)


def left(v):
    return lax.ppermute(v, "dp", LEFT)


def collect(block, ready=None):
    half = _half(block.shape[0])
    r = l = block
    got = [block]
    for s in (1, 2, 3, 4):
        if ready and s in ready:
            r, ready[s] = lax.optimization_barrier((r, ready[s]))
        r, l = (r, l) if s < 4 else (r[:half], l[half:])
        r, l = right(r), left(l)
        got += [r, l]
    return got


def rows_of(total, place, rows):
    return lax.dynamic_slice(total, (place * rows, jnp.int32(0)), (rows, total.shape[1]))


def scatter(term):
    add = lambda a, b: (a.astype(F32) + b.astype(F32)).astype(BF16)
    t = term(4)
    half = _half(t.shape[0])
    r, l = right(t[:half]), left(t[half:])
    a, b = term(3), term(-3)
    r, l = jnp.concatenate([add(r, a[:half]), a[half:]]), jnp.concatenate([b[:half], add(l, b[half:])])
    r, l = right(r), left(l)
    for s in (2, 1):
        r, l = add(r, term(s)), add(l, term(-s))
        r, l = right(r), left(l)
    return (term(0).astype(F32) + r.astype(F32) + l.astype(F32)).astype(BF16)


def across(v):
    return lax.ppermute(v, "tp", ACROSS)


def beside(v):
    return lax.ppermute(v, "tp", BESIDE)


def gathered(v):
    far = across(v)
    return [v, beside(v), far, beside(far)]


def joined(terms):
    t3, t2, t1, t0 = terms
    pair = beside(t3).astype(F32) + t2.astype(F32)
    pair = across(pair.astype(BF16))
    return t0.astype(F32) + beside(t1).astype(F32) + pair.astype(F32)


def terms_of(a, w, cb=1):
    return [lax.optimization_barrier(matmul(a[p * BLOCK : (p + 1) * BLOCK], w, cb=cb)) for p in (3, 2, 1, 0)]


def terms_by_chip(a, w):
    far, near = (lax.optimization_barrier(matmul(a[p * BLOCK : (p + 2) * BLOCK], w, cb=1)) for p in (2, 0))
    return [far[BLOCK:], far[:BLOCK], near[BLOCK:], near[:BLOCK]]


def matmul(a, w, ca=1, cb=0):
    return dot(a, w, ca, cb).astype(BF16)


def step(x, dy, wq, wk, wv, wo, w_gate, w_up, w_down):
    return layer(x[0], dy[0], wq, wk, wv, wo, w_gate, w_up, w_down)


def layer(x, dy, wq, wk, wv, wo, w_gate, w_up, w_down):
    me = lax.axis_index("tp").astype(jnp.int32)
    pos = ring(lax.axis_index("dp").astype(jnp.int32))
    at = jnp.stack([me, pos])
    c, f = wq.shape[1], w_gate.shape[1] // 2

    place = jnp.arange(4 * BLOCK, dtype=F32)[:, None] * THETA ** (-jnp.arange(HEAD // 2, dtype=F32) / (HEAD // 2))
    cos, sin = jnp.cos(place), jnp.sin(place)
    ready = {3: (jnp.concatenate([cos, cos], 1), jnp.concatenate([-sin, sin], 1)),
             4: tuple(jnp.concatenate([w_gate[:, n : n + f], w_up[:, n : n + f]], 1) for n in (0, f))}
    q_parts = collect(jnp.concatenate([wq, wk, wv], 1), ready)
    (cos, sin), (ua, ub) = ready[3], ready[4]
    a, norm_a = jax.vjp(normed, x)
    a = gathered(a)
    o_parts = collect(wo)
    y = gathered(dy)
    d_parts = collect(w_down)
    ua_parts = collect(ua)
    ub_parts = collect(ub)

    heads, rot, lse, a_full, wqkv, wo_full = attend(at, a, q_parts, o_parts, cos, sin)
    h = x + joined(terms_of(heads, wo_full, 0)).astype(BF16)
    b, norm_b = jax.vjp(normed, h)
    b = gathered(b)
    dhid, dyf = hidden_grad(at, y, d_parts)
    hid1, dgu, wgu, b_full = gated(at, b, ua_parts, dhid)
    by_down1 = matmul(hid1, dyf, 0, 0)
    hid2, dgu, wgu = gated(at, b, ub_parts, dhid, (dgu, wgu))
    by_down2 = matmul(hid2, dyf, 0, 0)
    rows = w_down.shape[0]

    def down_term(far):
        place = ring(pos + far)
        return jnp.where(place < 4, rows_of(by_down1, place, rows), rows_of(by_down2, place - 4, rows))

    of = lambda total: lambda far: rows_of(total, ring(pos + far), total.shape[0] // 8)
    by_down = scatter(down_term)
    dh = dy + norm_b(joined(terms_by_chip(dgu, wgu)).astype(BF16))[0]
    by_ua = scatter(of(matmul(b_full, dgu[:, : 2 * f], 0, 0)))
    by_ub = scatter(of(matmul(b_full, dgu[:, 2 * f :], 0, 0)))
    dhs = gathered(dh)
    near, far = jnp.concatenate(dhs[:2]), jnp.concatenate(dhs[2:])
    do_near, do_far = matmul(near, wo_full, cb=1), matmul(far, wo_full, cb=1)
    wo_near = lax.optimization_barrier(dot(heads[: 2 * BLOCK], near, 0, 0))
    wo_far = lax.optimization_barrier(dot(heads[2 * BLOCK :], far, 0, 0))
    by_wo = lax.optimization_barrier((wo_near + wo_far).astype(BF16).reshape(wq.shape[0] * 8, c))
    dqkv = attend_bwd(at, rot, heads, jnp.concatenate([do_near, do_far]), lse, cos, sin)
    by_qkv = matmul(a_full, dqkv, 0, 0)
    by_qkv = scatter(lambda far: jnp.concatenate([of(by_qkv)(far), of(by_wo)(far)], 1))
    da = joined(terms_of(dqkv, wqkv))
    dx = dh + norm_a(da.astype(BF16))[0]
    by_gate, by_up = (jnp.concatenate([by_ua[:, k : k + f], by_ub[:, k : k + f]], 1) for k in (0, f))
    return (dx[None], by_qkv[:, :c], by_qkv[:, c : 2 * c], by_qkv[:, 2 * c : 3 * c], by_qkv[:, 3 * c :].reshape(wo.shape), by_gate, by_up, by_down)


def solution(mesh):
    states, by_columns, by_rows = P("dp", "tp", None), P("dp", "tp"), P(("tp", "dp"), None)
    weights = (by_columns, by_columns, by_columns, by_rows, by_columns, by_columns, by_rows)
    return jax.shard_map(step, mesh=mesh, in_specs=(states, states, *weights), out_specs=(states, *weights), check_vma=False)
```

```python
import functools

import jax
import jax.numpy as jnp
from jax import lax
from jax.experimental import pallas as pl
from jax.experimental.pallas import tpu as pltpu
from jax.sharding import PartitionSpec as P


NEG = -1e30
HIDDEN = 2 * NEG
LOG2E = 1.4426950408889634
HEAD = 128
THETA = 10000
BLOCK = 512
VMEM = 36 * 2**20
F32, BF16 = jnp.float32, jnp.bfloat16


def dot(a, b, ca=1, cb=0):
    return lax.dot_general(a, b, (((ca,), (cb,)), ((), ())), preferred_element_type=F32)


def normed(h):
    wide = h.astype(F32)
    scale = lax.rsqrt(jnp.mean(wide**2, -1, keepdims=True) + 1e-6)
    return (wide * scale).astype(BF16)


def _mask():
    return lax.broadcasted_iota(jnp.int32, (BLOCK, BLOCK), 1) >= lax.broadcasted_iota(jnp.int32, (BLOCK, BLOCK), 0)


def _turn(t, cos, sin):
    return t * cos + pltpu.roll(t, HEAD // 2, 1) * sin


RING = [0, 1, 2, 3, 7, 6, 5, 4]
PIECES = [(0, 0), (-1, 0), (1, 0), (-2, 0), (2, 0), (-3, 0), (3, 0), (4, 0), (4, 1)]


def ring(q):
    q = lax.rem(q + 16, 8)
    return jnp.where(q < 4, q, 11 - q)


def _half(rows):
    return rows // 2 // 16 * 16


def _place(refs, to, sems, pos, columns=None):
    rows = refs[0].shape[0]
    copies = []
    for n, (ref, (far, second)) in enumerate(zip(refs, PIECES)):
        at = pl.multiple_of(ring(pos + far) * rows + second * _half(rows), 16)
        source, target = (ref, to.at[pl.ds(at, ref.shape[0]), :])
        if columns is not None:
            source, target = ref.at[:, columns], to.at[pl.ds(at, ref.shape[0]), columns]
        copies.append(pltpu.make_async_copy(source, target, sems.at[n]))
    return copies


def _side_by_side(*refs):
    for n, ref in enumerate(refs[:-1]):
        refs[-1][:, n * ref.shape[1] : (n + 1) * ref.shape[1]] = ref[...]


def side_by_side(*blocks):
    rows, c = blocks[0].shape
    return pl.pallas_call(
        _side_by_side, in_specs=[pl.BlockSpec((rows, c), lambda: (0, 0))] * len(blocks), out_specs=pl.BlockSpec((rows, len(blocks) * c), lambda: (0, 0)),
        out_shape=jax.ShapeDtypeStruct((rows, len(blocks) * c), BF16),
    )(*blocks)


def _stack(refs, to, sems):
    return [pltpu.make_async_copy(ref, to.at[pl.ds(n * BLOCK, BLOCK), :], sems.at[n]) for n, ref in enumerate(refs)]


def _attend(at_ref, *refs, heads):
    a_refs, w_refs, p_refs = refs[:4], refs[4:13], refs[13:22]
    cos_ref, sin_ref, o_ref, rot_ref, lse_ref, a_out, w_out, p_out, a_s, w_s, p_s, k_s, v_s, top_s, mix_s, a_sem, w_sem, p_sem, out_sem = refs[22:]
    iq = pl.program_id(0)
    me, pos = at_ref[0], at_ref[1]
    scale = HEAD**-0.5
    e = scale * LOG2E
    wide = heads * HEAD
    keep = [pltpu.make_async_copy(a, b, out_sem.at[n]) for n, (a, b) in enumerate(((a_s, a_out), (w_s, w_out), (p_s, p_out)))]

    @pl.when(iq == 0)
    def _():
        copies = _stack(a_refs, a_s, a_sem) + _place(w_refs, w_s, w_sem, pos) + _place(p_refs, p_s, p_sem, pos)
        for c in copies:
            c.start()
        for c in copies:
            c.wait()
        for c in keep:
            c.start()

    rows = pl.ds(pl.multiple_of((iq ^ me) * BLOCK, BLOCK), BLOCK)
    qkv = dot(a_s[rows, :], w_s[...]).astype(BF16)
    cos, sin = cos_ref[...], sin_ref[...]
    ones = jnp.ones((8, BLOCK), BF16)
    for i in range(heads):
        at = i * HEAD
        q = _turn(qkv[:, at : at + HEAD].astype(F32), cos, sin).astype(BF16)
        k = _turn(qkv[:, wide + at : wide + at + HEAD].astype(F32), cos, sin).astype(BF16)
        v = qkv[:, 2 * wide + at : 2 * wide + at + HEAD]
        rot_ref[:, at : at + HEAD] = q
        rot_ref[:, wide + at : wide + at + HEAD] = k
        rot_ref[:, 2 * wide + at : 2 * wide + at + HEAD] = v
        k_s[iq, :, at : at + HEAD] = k
        v_s[iq, i] = jnp.concatenate([v.T, ones], axis=0)
        top_s[i : i + 1, :] = jnp.full((1, BLOCK), NEG, F32)
        mix_s[i] = jnp.zeros((HEAD + 8, BLOCK), F32)

    def block(j, masked):
        scores = [dot(k_s[j, :, i * HEAD : (i + 1) * HEAD], rot_ref[:, i * HEAD : (i + 1) * HEAD], 1, 1) for i in range(heads)]
        ok = _mask() if masked else None
        weights, keeps = [], []
        for i, s in enumerate(scores):
            if masked:
                s = jnp.where(ok, s, HIDDEN)
            old = top_s[i : i + 1, :]
            top = jnp.maximum(old, s.max(axis=0, keepdims=True))
            top_s[i : i + 1, :] = top
            weights.append(jnp.exp2((s - top) * e).astype(BF16))
            keeps.append(jnp.exp2((old - top) * e))
        for i in range(heads):
            mix_s[i] = mix_s[i] * keeps[i] + dot(v_s[j, i], weights[i], 1, 0)

    lax.fori_loop(0, iq, lambda j, _: block(j, False), None)
    block(iq, True)
    for i in range(heads):
        total = mix_s[i, HEAD : HEAD + 1, :]
        o_ref[:, i * HEAD : (i + 1) * HEAD] = (mix_s[i, :HEAD, :] * (1 / total)).T.astype(BF16)
        lse_ref[i : i + 1, :] = top_s[i : i + 1, :] * scale + jnp.log(total)

    @pl.when(iq == pl.num_programs(0) - 1)
    def _():
        for c in keep:
            c.wait()


ANY = pl.BlockSpec(memory_space=pl.ANY)


def attend(at, blocks, pieces, o_pieces, cos, sin):
    n, d = len(blocks), blocks[0].shape[1]
    deep = 8 * o_pieces[0].shape[0]
    tokens, width = n * BLOCK, pieces[0].shape[1]
    heads = width // (3 * HEAD)
    here = lambda t, at: (t ^ at[0], 0)
    table = pl.BlockSpec((BLOCK, HEAD), lambda t, at: (t, 0))
    return pl.pallas_call(
        lambda *refs: _attend(*refs, heads=heads),
        grid_spec=pltpu.PrefetchScalarGridSpec(
            num_scalar_prefetch=1,
            grid=(n,),
            in_specs=[ANY] * 22 + [table, table],
            out_specs=[pl.BlockSpec((BLOCK, heads * HEAD), here), pl.BlockSpec((BLOCK, width), here),
                       pl.BlockSpec((heads, BLOCK), lambda t, at: (0, t ^ at[0])), ANY, ANY, ANY],
            scratch_shapes=[pltpu.VMEM((tokens, d), BF16), pltpu.VMEM((d, width), BF16), pltpu.VMEM((deep, d), BF16),
                            pltpu.VMEM((n, BLOCK, heads * HEAD), BF16), pltpu.VMEM((n, heads, HEAD + 8, BLOCK), BF16),
                            pltpu.VMEM((heads, BLOCK), F32), pltpu.VMEM((heads, HEAD + 8, BLOCK), F32),
                            pltpu.SemaphoreType.DMA((4,)), pltpu.SemaphoreType.DMA((9,)), pltpu.SemaphoreType.DMA((9,)), pltpu.SemaphoreType.DMA((3,))],
        ),
        out_shape=[jax.ShapeDtypeStruct((tokens, heads * HEAD), BF16), jax.ShapeDtypeStruct((tokens, width), BF16),
                   jax.ShapeDtypeStruct((heads, tokens), F32), jax.ShapeDtypeStruct((tokens, d), BF16), jax.ShapeDtypeStruct((d, width), BF16),
                   jax.ShapeDtypeStruct((deep, d), BF16)],
        compiler_params=pltpu.CompilerParams(dimension_semantics=("arbitrary",), vmem_limit_bytes=VMEM),
        cost_estimate=pl.CostEstimate(flops=2 * heads * tokens * tokens * HEAD * 3 + 2 * tokens * d * width, transcendentals=heads * tokens * tokens // 2,
                                      bytes_accessed=tokens * width * 5),
    )(at, *blocks, *pieces, *o_pieces, cos, sin)


def _hidden_grad(at_ref, *refs):
    y_refs, w_refs, out_ref, y_out, y_s, w_s, y_sem, w_sem, out_sem = refs[:4], refs[4:13], *refs[13:]
    m = pl.program_id(0)
    keep = pltpu.make_async_copy(y_s, y_out, out_sem)

    @pl.when(m == 0)
    def _():
        copies = _stack(y_refs, y_s, y_sem) + _place(w_refs, w_s, w_sem, at_ref[1])
        for c in copies:
            c.start()
        for c in copies:
            c.wait()
        keep.start()

    rows = pl.ds(pl.multiple_of(m * BLOCK, BLOCK), BLOCK)
    y = y_s[rows, :]
    tile = 512
    for n in range(0, out_ref.shape[1], tile):
        out_ref[:, n : n + tile] = dot(y, w_s[n : n + tile, :], 1, 1).astype(BF16)

    @pl.when(m == pl.num_programs(0) - 1)
    def _():
        keep.wait()


def hidden_grad(at, blocks, pieces):
    d = blocks[0].shape[1]
    tokens, ff = 4 * BLOCK, 8 * pieces[0].shape[0]
    return pl.pallas_call(
        _hidden_grad,
        grid_spec=pltpu.PrefetchScalarGridSpec(
            num_scalar_prefetch=1, grid=(4,), in_specs=[ANY] * 13, out_specs=[pl.BlockSpec((BLOCK, ff), lambda m, at: (m, 0)), ANY],
            scratch_shapes=[pltpu.VMEM((tokens, d), BF16), pltpu.VMEM((ff, d), BF16),
                            pltpu.SemaphoreType.DMA((4,)), pltpu.SemaphoreType.DMA((9,)), pltpu.SemaphoreType.DMA(())]),
        out_shape=[jax.ShapeDtypeStruct((tokens, ff), BF16), jax.ShapeDtypeStruct((tokens, d), BF16)],
        compiler_params=pltpu.CompilerParams(dimension_semantics=("arbitrary",), vmem_limit_bytes=VMEM),
        cost_estimate=pl.CostEstimate(flops=2 * tokens * ff * d, transcendentals=0, bytes_accessed=2 * tokens * (ff + 2 * d)),
    )(at, *blocks, *pieces)


def _attend_bwd(me_ref, rot_ref, o_ref, do_ref, lse_ref, cos_ref, sin_ref, out_ref, dq_s, dk_s, dv_s, *, heads, n):
    t = pl.program_id(0)
    iq = n - 1 - t
    me = me_ref[0]
    cos, sin = cos_ref[...], sin_ref[...]
    scale = HEAD**-0.5
    e = scale * LOG2E
    wide = heads * HEAD

    @pl.when(t == 0)
    def _():
        dk_s[...] = jnp.zeros_like(dk_s)
        dv_s[...] = jnp.zeros_like(dv_s)

    dq_s[...] = jnp.zeros_like(dq_s)
    mine = pl.ds((iq ^ me) * BLOCK, BLOCK)
    lses, deltas = [], []
    for i in range(heads):
        cut = slice(i * HEAD, (i + 1) * HEAD)
        lses.append(lse_ref[i : i + 1, :] * LOG2E)
        deltas.append((do_ref[:, cut].astype(F32) * o_ref[:, cut].astype(F32)).T.sum(axis=0, keepdims=True))

    def block(j, masked):
        keys = pl.ds((j ^ me) * BLOCK, BLOCK)
        cuts = [slice(i * HEAD, (i + 1) * HEAD) for i in range(heads)]
        qs = [rot_ref[mine, c] for c in cuts]
        ks = [rot_ref[keys, wide + i * HEAD : wide + (i + 1) * HEAD] for i in range(heads)]
        vs = [rot_ref[keys, 2 * wide + i * HEAD : 2 * wide + (i + 1) * HEAD] for i in range(heads)]
        scores = [dot(k, q, 1, 1) for k, q in zip(ks, qs)]
        dps = [dot(v, do_ref[:, c], 1, 1) for v, c in zip(vs, cuts)]
        ok = _mask() if masked else None
        for i in range(heads):
            p = jnp.exp2(scores[i] * e - lses[i])
            if masked:
                p = jnp.where(ok, p, 0.0)
            ds = (p * (dps[i] - deltas[i])).astype(BF16)
            dv_s[j, :, cuts[i]] += dot(p.astype(BF16), do_ref[:, cuts[i]], 1, 0)
            dk_s[j, :, cuts[i]] += dot(ds, qs[i], 1, 0)
            dq_s[i] += dot(ks[i].T, ds, 1, 0)

    lax.fori_loop(0, iq, lambda j, _: block(j, False), None)
    block(iq, True)
    for i in range(heads):
        cut = slice(i * HEAD, (i + 1) * HEAD)
        dq = (dq_s[i] * scale).T
        dk = dk_s[iq, :, cut] * scale
        out_ref[:, cut] = _turn(dq, cos, -sin).astype(BF16)
        out_ref[:, wide + i * HEAD : wide + (i + 1) * HEAD] = _turn(dk, cos, -sin).astype(BF16)
        out_ref[:, 2 * wide + i * HEAD : 2 * wide + (i + 1) * HEAD] = dv_s[iq, :, cut].astype(BF16)


def attend_bwd(me, rot, o, do, lse, cos, sin):
    tokens, width = rot.shape
    heads = width // (3 * HEAD)
    n = tokens // BLOCK
    here = lambda t, me: ((n - 1 - t) ^ me[0], 0)
    table = pl.BlockSpec((BLOCK, HEAD), lambda t, me: (n - 1 - t, 0))
    return pl.pallas_call(
        lambda *refs: _attend_bwd(*refs, heads=heads, n=n),
        grid_spec=pltpu.PrefetchScalarGridSpec(
            num_scalar_prefetch=1,
            grid=(n,),
            in_specs=[pl.BlockSpec((tokens, width), lambda t, me: (0, 0)), pl.BlockSpec((BLOCK, heads * HEAD), here),
                      pl.BlockSpec((BLOCK, heads * HEAD), here), pl.BlockSpec((heads, BLOCK), lambda t, me: (0, (n - 1 - t) ^ me[0])),
                      table, table],
            out_specs=pl.BlockSpec((BLOCK, width), here),
            scratch_shapes=[pltpu.VMEM((heads, HEAD, BLOCK), F32), pltpu.VMEM((n, BLOCK, heads * HEAD), F32),
                            pltpu.VMEM((n, BLOCK, heads * HEAD), F32)],
        ),
        out_shape=jax.ShapeDtypeStruct((tokens, width), BF16),
        compiler_params=pltpu.CompilerParams(dimension_semantics=("arbitrary",), vmem_limit_bytes=VMEM),
        cost_estimate=pl.CostEstimate(flops=2 * heads * tokens * tokens * HEAD * 4, transcendentals=heads * tokens * tokens // 2,
                                      bytes_accessed=tokens * width * 5),
    )(me, rot, o, do, lse, cos, sin)


def _gated(at_ref, *refs, second):
    b_refs, w_refs, dh_ref, rest = refs[:4], refs[4:13], refs[13], refs[14 + 2 * second :]
    hid_ref, dgu_ref, w_out, *b_out, b_s, w_s, b_sem, w_sem, out_sem = rest
    m = pl.program_id(0)
    half, wide = dh_ref.shape[1], w_s.shape[1]
    blocks = _stack(b_refs, b_s, b_sem)
    weights = _place(w_refs, w_s, w_sem, at_ref[1])
    keep = [pltpu.make_async_copy(w_s, w_out.at[:, second * wide : (second + 1) * wide], out_sem.at[0])]
    late = [pltpu.make_async_copy(b_s, out, out_sem.at[1]) for out in b_out]

    @pl.when(m == 0)
    def _():
        for c in [blocks[0]] + weights + blocks[1:]:
            c.start()
        for c in weights:
            c.wait()
        for c in keep:
            c.start()

    for k, c in enumerate(blocks):

        @pl.when(m == k)
        def _():
            c.wait()
            if k == len(blocks) - 1:
                for o in late:
                    o.start()

    part = BLOCK // 2
    for i in range(2):
        here = slice(i * part, (i + 1) * part)
        both = dot(b_s[pl.ds(pl.multiple_of(m * BLOCK + i * part, part), part), :], w_s[...])
        gate, up = both[:, :half], both[:, half:]
        dh = dh_ref[here, :].astype(F32)
        sig = 1 / (1 + jnp.exp(-gate))
        silu = gate * sig
        hid_ref[here, :] = (silu * up).astype(BF16)
        dgu_ref[here, :half] = (dh * up * (sig * (1 + gate * (1 - sig)))).astype(BF16)
        dgu_ref[here, half:] = (dh * silu).astype(BF16)

    @pl.when(m == pl.num_programs(0) - 1)
    def _():
        for c in keep + late:
            c.wait()


def gated(at, blocks, pieces, dhid, earlier=()):
    d, (tokens, ff) = blocks[0].shape[1], dhid.shape
    second, half = len(earlier) // 2, ff // 2
    outs = [jax.ShapeDtypeStruct((tokens, half), BF16), jax.ShapeDtypeStruct((tokens, 2 * ff), BF16), jax.ShapeDtypeStruct((d, 2 * ff), BF16)]
    outs += [] if second else [jax.ShapeDtypeStruct((tokens, d), BF16)]
    return pl.pallas_call(
        functools.partial(_gated, second=second),
        grid_spec=pltpu.PrefetchScalarGridSpec(
            num_scalar_prefetch=1,
            grid=(tokens // BLOCK,),
            in_specs=[ANY] * 13 + [pl.BlockSpec((BLOCK, half), lambda m, at: (m, second))] + [ANY] * len(earlier),
            out_specs=[pl.BlockSpec((BLOCK, half), lambda m, at: (m, 0)), pl.BlockSpec((BLOCK, ff), lambda m, at: (m, second))] + [ANY] * (len(outs) - 2),
            scratch_shapes=[pltpu.VMEM((tokens, d), BF16), pltpu.VMEM((d, ff), BF16),
                            pltpu.SemaphoreType.DMA((4,)), pltpu.SemaphoreType.DMA((9,)), pltpu.SemaphoreType.DMA((2,))],
        ),
        out_shape=outs,
        input_output_aliases={15 + n: 1 + n for n in range(len(earlier))},
        compiler_params=pltpu.CompilerParams(dimension_semantics=("arbitrary",), vmem_limit_bytes=VMEM),
        cost_estimate=pl.CostEstimate(flops=2 * tokens * d * ff, transcendentals=tokens * half, bytes_accessed=2 * (tokens * d + d * ff + 2 * tokens * ff)),
    )(at, *blocks, *pieces, dhid, *earlier)


RIGHT = [(RING[i], RING[(i + 1) % 8]) for i in range(8)]
LEFT = [(b, a) for a, b in RIGHT]
ACROSS = [(i, i ^ 2) for i in range(4)]
BESIDE = [(i, i ^ 1) for i in range(4)]


def right(v):
    return lax.ppermute(v, "dp", RIGHT)


def left(v):
    return lax.ppermute(v, "dp", LEFT)


def collect(block, ready=None):
    half = _half(block.shape[0])
    r = l = block
    got = [block]
    for s in (1, 2, 3, 4):
        if ready and s in ready:
            r, ready[s] = lax.optimization_barrier((r, ready[s]))
        r, l = (r, l) if s < 4 else (r[:half], l[half:])
        r, l = right(r), left(l)
        got += [r, l]
    return got


def rows_of(total, place, rows):
    return lax.dynamic_slice(total, (place * rows, jnp.int32(0)), (rows, total.shape[1]))


def scatter(term):
    add = lambda a, b: (a.astype(F32) + b.astype(F32)).astype(BF16)
    t = term(4)
    half = _half(t.shape[0])
    r, l = right(t[:half]), left(t[half:])
    a, b = term(3), term(-3)
    r, l = jnp.concatenate([add(r, a[:half]), a[half:]]), jnp.concatenate([b[:half], add(l, b[half:])])
    r, l = right(r), left(l)
    for s in (2, 1):
        r, l = add(r, term(s)), add(l, term(-s))
        r, l = right(r), left(l)
    return (term(0).astype(F32) + r.astype(F32) + l.astype(F32)).astype(BF16)


def across(v):
    return lax.ppermute(v, "tp", ACROSS)


def beside(v):
    return lax.ppermute(v, "tp", BESIDE)


def gathered(v):
    far = across(v)
    return [v, beside(v), far, beside(far)]


def joined(terms):
    t3, t2, t1, t0 = terms
    pair = beside(t3).astype(F32) + t2.astype(F32)
    pair = across(pair.astype(BF16))
    return t0.astype(F32) + beside(t1).astype(F32) + pair.astype(F32)


def terms_of(a, w, cb=1):
    return [lax.optimization_barrier(matmul(a[p * BLOCK : (p + 1) * BLOCK], w, cb=cb)) for p in (3, 2, 1, 0)]


def terms_by_chip(a, w):
    far, near = (lax.optimization_barrier(matmul(a[p * BLOCK : (p + 2) * BLOCK], w, cb=1)) for p in (2, 0))
    return [far[BLOCK:], far[:BLOCK], near[BLOCK:], near[:BLOCK]]


def matmul(a, w, ca=1, cb=0):
    return dot(a, w, ca, cb).astype(BF16)


def step(x, dy, wq, wk, wv, wo, w_gate, w_up, w_down):
    return layer(x[0], dy[0], wq, wk, wv, wo, w_gate, w_up, w_down)


def layer(x, dy, wq, wk, wv, wo, w_gate, w_up, w_down):
    me = lax.axis_index("tp").astype(jnp.int32)
    pos = ring(lax.axis_index("dp").astype(jnp.int32))
    at = jnp.stack([me, pos])
    c, f = wq.shape[1], w_gate.shape[1] // 2

    place = jnp.arange(4 * BLOCK, dtype=F32)[:, None] * THETA ** (-jnp.arange(HEAD // 2, dtype=F32) / (HEAD // 2))
    cos, sin = jnp.cos(place), jnp.sin(place)
    ready = {3: (jnp.concatenate([cos, cos], 1), jnp.concatenate([-sin, sin], 1)),
             4: tuple(jnp.concatenate([w_gate[:, n : n + f], w_up[:, n : n + f]], 1) for n in (0, f))}
    q_parts = collect(side_by_side(wq, wk, wv), ready)
    (cos, sin), (ua, ub) = ready[3], ready[4]
    a, norm_a = jax.vjp(normed, x)
    a = gathered(a)
    o_parts = collect(wo)
    y = gathered(dy)
    d_parts = collect(w_down)
    ua_parts = collect(ua)
    ub_parts = collect(ub)

    heads, rot, lse, a_full, wqkv, wo_full = attend(at, a, q_parts, o_parts, cos, sin)
    h = x + joined(terms_of(heads, wo_full, 0)).astype(BF16)
    b, norm_b = jax.vjp(normed, h)
    b = gathered(b)
    dhid, dyf = hidden_grad(at, y, d_parts)
    hid1, dgu, wgu, b_full = gated(at, b, ua_parts, dhid)
    by_down1 = matmul(hid1, dyf, 0, 0)
    hid2, dgu, wgu = gated(at, b, ub_parts, dhid, (dgu, wgu))
    by_down2 = matmul(hid2, dyf, 0, 0)
    rows = w_down.shape[0]

    def down_term(far):
        place = ring(pos + far)
        return jnp.where(place < 4, rows_of(by_down1, place, rows), rows_of(by_down2, place - 4, rows))

    of = lambda total: lambda far: rows_of(total, ring(pos + far), total.shape[0] // 8)
    by_down = scatter(down_term)
    dh = dy + norm_b(joined(terms_by_chip(dgu, wgu)).astype(BF16))[0]
    by_ua = scatter(of(matmul(b_full, dgu[:, : 2 * f], 0, 0)))
    by_ub = scatter(of(matmul(b_full, dgu[:, 2 * f :], 0, 0)))
    dhs = gathered(dh)
    near, far = jnp.concatenate(dhs[:2]), jnp.concatenate(dhs[2:])
    do_near, do_far = matmul(near, wo_full, cb=1), matmul(far, wo_full, cb=1)
    wo_near = lax.optimization_barrier(dot(heads[: 2 * BLOCK], near, 0, 0))
    wo_far = lax.optimization_barrier(dot(heads[2 * BLOCK :], far, 0, 0))
    by_wo = lax.optimization_barrier((wo_near + wo_far).astype(BF16).reshape(wq.shape[0] * 8, c))
    dqkv = attend_bwd(at, rot, heads, jnp.concatenate([do_near, do_far]), lse, cos, sin)
    by_qkv = matmul(a_full, dqkv, 0, 0)
    by_qkv = scatter(lambda far: jnp.concatenate([of(by_qkv)(far), of(by_wo)(far)], 1))
    da = joined(terms_of(dqkv, wqkv))
    dx = dh + norm_a(da.astype(BF16))[0]
    by_gate, by_up = (jnp.concatenate([by_ua[:, k : k + f], by_ub[:, k : k + f]], 1) for k in (0, f))
    return (dx[None], by_qkv[:, :c], by_qkv[:, c : 2 * c], by_qkv[:, 2 * c : 3 * c], by_qkv[:, 3 * c :].reshape(wo.shape), by_gate, by_up, by_down)


def solution(mesh):
    states, by_columns, by_rows = P("dp", "tp", None), P("dp", "tp"), P(("tp", "dp"), None)
    weights = (by_columns, by_columns, by_columns, by_rows, by_columns, by_columns, by_rows)
    return jax.shard_map(step, mesh=mesh, in_specs=(states, states, *weights), out_specs=(states, *weights), check_vma=False)
```
